256 devices in a mesh: dp: 16 (over z_lo, y), mp: 16 (over x, z_hi, core).
Axes of the slice: x: 4, y: 4, z: 8 (z_hi: 2, z_lo: 4; z = z_hi * 4 + z_lo), core: 2. Of those that a mesh axis runs over, the one named last changes fastest.
Arguments:
- image_tokens: bfloat16 [16, 192, 3072], P('dp'), may hold values from -6 to 6
- text_tokens: bfloat16 [16, 64, 3072], P('dp'), may hold values from -6 to 6
- null_prompt: bfloat16 [64, 3072], replicated, may hold values from -6 to 6
- drop_flags: int32 [16], P('dp'), may hold values 0 or 1
- time_index: int32 [16], P('dp'), may hold values from 0 to 31
- modulation: float32 [32, 3, 3072], replicated, may hold values from -3 to 3
- w_up: bfloat16 [3072, 12288], P('dp', 'mp'), may hold values from -0.109375 to 0.109375
- w_down: bfloat16 [12288, 3072], P('mp', 'dp'), may hold values from -0.0546875 to 0.0546875
- d_output: bfloat16 [16, 256, 3072], P('dp'), may hold values from -6 to 6
Outputs:
- block_out: bfloat16 [16, 256, 3072], P('dp')
- d_tokens: bfloat16 [16, 256, 3072], P('dp')
- grad_up: float32 [3072, 12288], P('dp', 'mp')
- grad_down: float32 [12288, 3072], P('mp', 'dp')
- grad_null: float32 [64, 3072], replicated
The draws below stay inside these ranges and needn't reach their ends.
All inputs are finite; a program needn't handle non-finite values. No bound on the sum of `drop_flags` on one device may be relied on, other than what follows from the above.
Results may differ from the reference program's by a relative error of at most 0.017.
Values may be sent and summed in bfloat16 or wider, within the bound.
No kernel may reach another device: no remote copies, remote signals or barrier semaphores. Data moves between devices by JAX's collectives and lax.ppermute only.
A program may use at most 128 MiB of HBM per device.

```python
import jax
import jax.numpy as jnp
from jax import lax

D = 3072
FF = 12288
L_IMG = 192
L_TXT = 64
NT = 32
B = 16
L = 256
N_MP = 16


def touch_ends(values, stream_key, low, largest):
    extent = values.shape
    place = [jax.random.randint(jax.random.fold_in(stream_key, axis), (), 0, extent[axis]) for axis in range(len(extent))]
    values = values.at[tuple(place)].set(low)
    longest = extent.index(max(extent))
    place[longest] = (place[longest] + 1) % extent[longest]
    return values.at[tuple(place)].set(largest)


def block_levels(key, shape, pieces, low, largest):
    gain = 1.0
    for axis_at, shards_of in pieces:
        heights = jax.random.uniform(jax.random.fold_in(jax.random.fold_in(key, 6), axis_at), (shards_of,), jnp.float32, low / len(pieces), largest / len(pieces))
        gain = gain * jnp.repeat(jnp.exp(heights), shape[axis_at] // shards_of).reshape((-1,) + (1,) * (len(shape) - 1 - axis_at))
    return gain


def gaussian(rng, dims, scale, most, shards=(), held_as=jnp.bfloat16):
    result = jax.random.normal(rng, dims, jnp.float32) * scale
    if len(shards) > 0:
        result = block_levels(rng, dims, shards, -0.22, 0.18) * result
    return jnp.clip(result, min=-most, max=most).astype(held_as)


def setup_inputs(seed: int = 0) -> dict:
    key_list = jax.random.split(jax.random.key(seed), 10)
    return {
        "image_tokens": gaussian(key_list[0], (B, L_IMG, D), 1.0, 6.0, ((0, 16),)),
        "text_tokens": gaussian(key_list[1], (B, L_TXT, D), 1.0, 6.0, ((0, 16),)),
        "null_prompt": gaussian(key_list[2], (L_TXT, D), 1.0, 6.0),
        "drop_flags": touch_ends((jax.random.randint(key_list[3], (B,), 0, 2) < 1).astype(jnp.int32), jax.random.fold_in(key_list[3], 1), 0, 1),
        "time_index": touch_ends(jax.random.randint(key_list[4], (B,), 0, NT), jax.random.fold_in(key_list[4], 1), 0, NT - 1).astype(jnp.int32),
        "modulation": gaussian(key_list[5], (NT, 3, D), 0.5, 3.0, (), jnp.float32),
        "w_up": gaussian(key_list[6], (D, FF), D ** -0.5, 0.109375, ((0, 16), (1, 16))),
        "w_down": gaussian(key_list[7], (FF, D), FF ** -0.5, 0.0546875, ((0, 16), (1, 16))),
        "d_output": gaussian(key_list[8], (B, L, D), 1.0, 6.0, ((0, 16),)),
    }


EPS = 1e-06

def gelu_tanh(values):
    return jax.nn.gelu(values, approximate=True)

def reference(image_tokens, text_tokens, null_prompt, drop_flags, time_index, modulation, w_up, w_down, d_output):
    dropped = drop_flags == 1
    text_in = jnp.where(dropped[:, None, None], null_prompt[None], text_tokens)
    joined = jnp.concatenate([text_in, image_tokens], axis=1)
    levels = jnp.arange(modulation.shape[0], dtype=jnp.int32)
    indicator_matrix = (time_index[:, None] == levels[None, :]).astype(jnp.float32)
    modulation_vectors = jnp.einsum('yi,imr->ymr', indicator_matrix, modulation.astype(jnp.float32), precision=lax.Precision.HIGHEST)
    shift_modulation = modulation_vectors[:, 0][:, None]
    scale_mod = modulation_vectors[:, 1][:, None]
    gate_mod = modulation_vectors[:, 2][:, None]
    batch, length, width = joined.shape
    joined32 = joined.astype(jnp.float32)
    centred = joined32 - lax.optimization_barrier(jnp.mean(joined32, axis=-1, keepdims=True))
    inv_std = lax.rsqrt(lax.optimization_barrier(jnp.mean(centred * centred, axis=-1, keepdims=True)) + EPS)
    normed = centred * inv_std
    mod_in = (normed * (1.0 + scale_mod) + shift_modulation).astype(jnp.bfloat16)
    flat_in = mod_in.reshape(batch * length, width)
    preactivation_rows = jnp.dot(flat_in, w_up, preferred_element_type=jnp.float32)
    hidden = gelu_tanh(preactivation_rows).astype(jnp.bfloat16)
    per_part = w_up.shape[1] // N_MP
    block_ids = jnp.arange(N_MP, dtype=jnp.int32)

    def add_branch(total, block_no):
        start = (block_no * per_part).astype(jnp.int32)
        cols = lax.dynamic_slice_in_dim(hidden, start, per_part, 1)
        rows_w = lax.dynamic_slice_in_dim(w_down, start, per_part, 0)
        part = jnp.dot(cols, rows_w, preferred_element_type=jnp.float32).astype(jnp.bfloat16)
        part = lax.optimization_barrier(part)
        return (total + part.astype(jnp.float32), None)
    branch, _ = lax.scan(add_branch, jnp.zeros((batch * length, width), jnp.float32), block_ids)
    branch = branch.reshape(batch, length, width)
    block_out = (joined32 + gate_mod * branch).astype(jnp.bfloat16)
    d_out32 = d_output.astype(jnp.float32)
    d_branch = (d_out32 * gate_mod).astype(jnp.bfloat16).reshape(batch * length, width)
    hidden_gradient = jnp.dot(d_branch, w_down.T, preferred_element_type=jnp.float32)
    _, gelu_back = jax.vjp(gelu_tanh, preactivation_rows)
    d_pre = gelu_back(hidden_gradient)[0].astype(jnp.bfloat16)
    grad_down = jnp.dot(hidden.T, d_branch, preferred_element_type=jnp.float32)
    grad_up = jnp.dot(flat_in.T, d_pre, preferred_element_type=jnp.float32)

    def add_input(total, block_no):
        start = (block_no * per_part).astype(jnp.int32)
        cols = lax.dynamic_slice_in_dim(d_pre, start, per_part, 1)
        wcols = lax.dynamic_slice_in_dim(w_up, start, per_part, 1)
        part = jnp.dot(cols, wcols.T, preferred_element_type=jnp.float32).astype(jnp.bfloat16)
        part = lax.optimization_barrier(part)
        return (total + part.astype(jnp.float32), None)
    d_mod, _ = lax.scan(add_input, jnp.zeros((batch * length, width), jnp.float32), block_ids)
    d_normed = d_mod.reshape(batch, length, width) * (1.0 + scale_mod)
    d_full = d_out32 + inv_std * (d_normed - lax.optimization_barrier(jnp.mean(d_normed, axis=-1, keepdims=True)) - normed * lax.optimization_barrier(jnp.mean(d_normed * normed, axis=-1, keepdims=True)))
    grad_null = lax.optimization_barrier(jnp.sum(jnp.where(dropped[:, None, None], d_full[:, :L_TXT], jnp.float32(0.0)), axis=0))
    return (block_out, d_full.astype(jnp.bfloat16), grad_up, grad_down, grad_null)
```

```python
import jax
import jax.numpy as jnp
from jax import lax
from jax.sharding import Mesh
from jax.sharding import PartitionSpec as P

EPS = 1e-06

G = 2

Z = ("zq", "zp")
DP = ("zq", "zp", "y")
MP = ("x", "zh", "c")
SLOT = ("c", "x")
NZ = 4
NY = 4


def exchange(pieces, axes):
    return lax.all_to_all(pieces, axes, 0, 0, tiled=True)


def spread(piece, axes, count):
    if count == 1:
        return piece[None]
    return exchange(jnp.broadcast_to(piece[None], (count, *piece.shape)), axes)


def summed(pieces):
    return jnp.sum(pieces.astype(jnp.float32), axis=0)


def gelu_tanh(values):
    return jax.nn.gelu(values, approximate=True)


def contract_rows(left, right):
    return lax.dot_general(
        left, right, (((0,), (0,)), ((), ())), preferred_element_type=jnp.float32
    )


def contract_cols(left, right):
    return lax.dot_general(
        left, right, (((1,), (1,)), ((), ())), preferred_element_type=jnp.float32
    )


def y_first(rows):
    n, d = rows.shape
    return rows.reshape(n, NZ, NY, -1).swapaxes(1, 2).reshape(n, d)


def z_first(rows):
    n, d = rows.shape
    return rows.reshape(n, NY, NZ, -1).swapaxes(1, 2).reshape(n, d)


def part_weights(weight):
    rows, hid = weight.shape
    cut = [weight[:, at : at + hid // G] for at in range(0, hid, hid // G)]
    sent = jnp.stack(cut * (NZ // G))
    got = exchange(sent, Z).reshape(NZ * rows, hid // G)
    return lax.all_gather(got, "y", axis=0, tiled=True)


def own_grads(grad):
    hid = grad.shape[1]
    mine = lax.psum_scatter(grad.astype(jnp.bfloat16), "y", scatter_dimension=0, tiled=True)
    rows = mine.shape[0] // NZ
    got = exchange(mine.reshape(NZ, rows, hid), Z).reshape(NZ // G, G, rows, hid)
    return jnp.concatenate([summed(got[:, part]) for part in range(G)], axis=1)


def own_slot(part):
    width = part.shape[1]
    half = summed(exchange(part.reshape(2, -1, width), "c")).astype(jnp.bfloat16)
    slot = summed(exchange(half.reshape(4, -1, width), "x")).astype(jnp.bfloat16)
    both = slot.reshape(G, 1, -1, width)
    both = jnp.broadcast_to(both, (G, 2, *both.shape[2:])).reshape(2 * G, -1, width)
    return z_first(summed(exchange(both, ("zp", "zh"))))


def whole_sample(slot, text):
    every = spread(slot, SLOT, 8)
    width = slot.shape[1]
    return jnp.concatenate(
        [every[:, :text].reshape(-1, width), every[:, text:].reshape(-1, width)], axis=0
    )[None]


def shards(
    image_tokens,
    text_tokens,
    null_prompt,
    drop_flags,
    time_index,
    modulation,
    w_up,
    w_down,
    d_output,
):
    width = null_prompt.shape[1]
    text_len = null_prompt.shape[0]
    text = text_len // 8
    image = image_tokens.shape[1] // 8
    place = lax.axis_index(SLOT)
    dropped = drop_flags[0] == 1

    full_up = part_weights(w_up)
    full_down = part_weights(w_down.T)

    def rows_of(array, start, count):
        return lax.dynamic_slice_in_dim(array, start, count, 0)

    joined32 = jnp.concatenate(
        [
            jnp.where(
                dropped,
                rows_of(null_prompt, place * text, text),
                rows_of(text_tokens[0], place * text, text),
            ),
            rows_of(image_tokens[0], place * image, image),
        ],
        axis=0,
    ).astype(jnp.float32)
    d_out32 = jnp.concatenate(
        [
            rows_of(d_output[0], place * text, text),
            rows_of(d_output[0], text_len + place * image, image),
        ],
        axis=0,
    ).astype(jnp.float32)
    vectors = lax.dynamic_index_in_dim(modulation, time_index[0], 0, keepdims=False)
    shift, scale, gate = vectors[0][None], vectors[1][None], vectors[2][None]
    centred = joined32 - jnp.mean(joined32, axis=-1, keepdims=True)
    inv_std = lax.rsqrt(jnp.mean(centred * centred, axis=-1, keepdims=True) + EPS)
    normed = centred * inv_std
    mod_slot = y_first((normed * (1.0 + scale) + shift).astype(jnp.bfloat16))
    back_slot = y_first((d_out32 * gate).astype(jnp.bfloat16))

    pair = spread(jnp.stack([mod_slot, back_slot]), "zp", G)
    mod_in = spread(pair[:, 0], SLOT, 8).reshape(-1, width)
    d_branch = spread(pair[:, 1], SLOT, 8).reshape(-1, width)

    pre = jnp.dot(mod_in, full_up, preferred_element_type=jnp.float32)
    hidden = gelu_tanh(pre).astype(jnp.bfloat16)
    grad_down = own_grads(contract_rows(d_branch, hidden)).T
    hidden_gradient = jnp.dot(d_branch, full_down, preferred_element_type=jnp.float32)
    _, gelu_back = jax.vjp(gelu_tanh, pre)
    d_pre = gelu_back(hidden_gradient)[0].astype(jnp.bfloat16)
    grad_up = own_grads(contract_rows(mod_in, d_pre))

    branch = own_slot(contract_cols(hidden, full_down).astype(jnp.bfloat16))
    block_out = whole_sample((joined32 + gate * branch).astype(jnp.bfloat16), text)

    d_mod = own_slot(contract_cols(d_pre, full_up).astype(jnp.bfloat16))
    d_normed = d_mod * (1.0 + scale)
    d_full = d_out32 + inv_std * (
        d_normed
        - jnp.mean(d_normed, axis=-1, keepdims=True)
        - normed * jnp.mean(d_normed * normed, axis=-1, keepdims=True)
    )
    d_tokens = whole_sample(d_full.astype(jnp.bfloat16), text)

    null_part = jnp.where(dropped, d_full[:text], jnp.float32(0.0)).astype(jnp.bfloat16)
    null_part = null_part.reshape(text, 16, -1).swapaxes(0, 1)
    null_own = summed(exchange(null_part, DP)).astype(jnp.bfloat16)
    null_rows = spread(null_own, DP, 16).swapaxes(0, 1).reshape(text, width)
    grad_null = spread(null_rows, SLOT, 8).reshape(text_len, width).astype(jnp.float32)
    return (block_out, d_tokens, grad_up, grad_down, grad_null)


def solution(mesh):
    torus = Mesh(
        mesh.devices.reshape(NZ // G, G, NY, 4, 2, 2), ("zq", "zp", "y", "x", "zh", "c")
    )
    in_specs = (
        P(DP, None, None),
        P(DP, None, None),
        P(),
        P(DP),
        P(DP),
        P(),
        P(DP, MP),
        P(MP, DP),
        P(DP, None, None),
    )
    out_specs = (P(DP, None, None), P(DP, None, None), P(DP, MP), P(MP, DP), P())
    return jax.shard_map(
        shards, mesh=torus, in_specs=in_specs, out_specs=out_specs, check_vma=False
    )
```

```python
import jax
import jax.numpy as jnp
from jax import lax
from jax.sharding import Mesh
from jax.sharding import PartitionSpec as P

EPS = 1e-06


Z = ("zq", "zp")
DP = ("zq", "zp", "y")
MP = ("x", "zh", "c")
SIZE = {Z: 4, "y": 4, "x": 4, "zp": 2, "zh": 2, "c": 2}
SLOTS = 8


def peer(value, axis, k):
    return lax.ppermute(value, axis, [(i, i ^ k) for i in range(SIZE[axis])])


def gathered(value, axis):
    return [value] + [peer(value, axis, k) for k in range(1, SIZE[axis])]


def ordered(pieces, axis):
    own = lax.axis_index(axis)
    return [lax.select_n(own ^ j, *pieces) if len(pieces) > 2 else
            jnp.where(own == j, pieces[0], pieces[1]) for j in range(len(pieces))]


def total(pieces):
    acc = pieces[0].astype(jnp.float32)
    for piece in pieces[1:]:
        acc = acc + piece.astype(jnp.float32)
    return acc


def rounded(value):
    return lax.reduce_precision(value, 8, 7).astype(jnp.bfloat16)


def gelu_tanh(values):
    return jax.nn.gelu(values, approximate=True)


def contract_rows(left, right):
    return lax.dot_general(
        left, right, (((0,), (0,)), ((), ())), preferred_element_type=jnp.float32
    )


def contract_cols(left, right):
    return lax.dot_general(
        left, right, (((1,), (1,)), ((), ())), preferred_element_type=jnp.float32
    )


def part_weights(weight):
    first = lax.axis_index("zp") == 0
    left, right = jnp.split(weight, 2, axis=1)
    mine = jnp.where(first, left, right)
    other = jnp.where(first, right, left)
    by_z = [mine, peer(other, Z, 1), peer(mine, Z, 2), peer(other, Z, 3)]
    block = jnp.stack(ordered(by_z, Z))
    by_y = gathered(block, "y")
    return jnp.concatenate(ordered(by_y, "y"), axis=1).reshape(-1, mine.shape[1])


def own_grads(grad):
    hid = grad.shape[1]
    blocks = grad.astype(jnp.bfloat16).reshape(4, 4, -1, hid)
    y = lax.axis_index("y")
    sent = [lax.dynamic_index_in_dim(blocks, y ^ k, 1, keepdims=False) for k in range(4)]
    block = rounded(total([sent[0]] + [peer(sent[k], "y", k) for k in range(1, 4)]))
    z = lax.axis_index(Z)
    sent = [lax.dynamic_index_in_dim(block, z ^ k, 0, keepdims=False) for k in range(4)]
    got = [sent[0]] + [peer(sent[k], Z, k) for k in range(1, 4)]
    mine, other = total([got[0], got[2]]), total([got[1], got[3]])
    first = lax.axis_index("zp") == 0
    return jnp.concatenate([jnp.where(first, mine, other), jnp.where(first, other, mine)], axis=1)


def group_tokens(pair):
    along_x = jnp.concatenate(gathered(pair, "x"), axis=0)
    return jnp.concatenate(gathered(along_x, "c"), axis=0).reshape(-1, pair.shape[-1])


def own_slot(part):
    width = part.shape[1]
    halves = part.reshape(2, -1, width)
    half = rounded(total([halves[0], peer(halves[1], "c", 1)])).reshape(4, -1, width)
    slot = rounded(total([half[0]] + [peer(half[k], "x", k) for k in range(1, 4)]))
    slot = slot.reshape(2, -1, width)
    own = rounded(total([slot[0], peer(slot[1], "zp", 1)]))
    return total([own, peer(own, "zh", 1)])


def all_slots(rows):
    along_x = jnp.stack(ordered(gathered(rows, "x"), "x"))
    return jnp.concatenate(ordered(gathered(along_x, "c"), "c"), axis=0)


def whole_sample(rows, text):
    every = all_slots(rows)
    width = rows.shape[1]
    return jnp.concatenate(
        [every[:, :text].reshape(-1, width), every[:, text:].reshape(-1, width)], axis=0
    )[None]


def shards(
    image_tokens,
    text_tokens,
    null_prompt,
    drop_flags,
    time_index,
    modulation,
    w_up,
    w_down,
    d_output,
):
    text_len, width = null_prompt.shape
    text = text_len // SLOTS
    image = image_tokens.shape[1] // SLOTS
    place = lax.axis_index(("c", "x"))
    dropped = drop_flags[0] == 1

    full_up = part_weights(w_up)
    full_down = part_weights(w_down.T)

    def rows_of(array, start, count):
        return lax.dynamic_slice_in_dim(array, start, count, 0)

    joined32 = jnp.concatenate(
        [
            jnp.where(
                dropped,
                rows_of(null_prompt, place * text, text),
                rows_of(text_tokens[0], place * text, text),
            ),
            rows_of(image_tokens[0], place * image, image),
        ],
        axis=0,
    ).astype(jnp.float32)
    d_out32 = jnp.concatenate(
        [
            rows_of(d_output[0], place * text, text),
            rows_of(d_output[0], text_len + place * image, image),
        ],
        axis=0,
    ).astype(jnp.float32)
    vectors = lax.dynamic_index_in_dim(modulation, time_index[0], 0, keepdims=False)
    shift, scale, gate = vectors[0][None], vectors[1][None], vectors[2][None]
    centred = joined32 - jnp.mean(joined32, axis=-1, keepdims=True)
    inv_std = lax.rsqrt(jnp.mean(centred * centred, axis=-1, keepdims=True) + EPS)
    normed = centred * inv_std
    mod_slot = (normed * (1.0 + scale) + shift).astype(jnp.bfloat16)
    back_slot = (d_out32 * gate).astype(jnp.bfloat16)

    both = jnp.stack([mod_slot, back_slot])
    partner = peer(both, "zp", 1)
    mod_in = group_tokens(jnp.stack([both[0], partner[0]]))
    d_branch = group_tokens(jnp.stack([both[1], partner[1]]))

    pre = jnp.dot(mod_in, full_up, preferred_element_type=jnp.float32)
    hidden = gelu_tanh(pre).astype(jnp.bfloat16)
    grad_down = own_grads(contract_rows(d_branch, hidden)).T
    hidden_gradient = jnp.dot(d_branch, full_down, preferred_element_type=jnp.float32)
    _, gelu_back = jax.vjp(gelu_tanh, pre)
    d_pre = gelu_back(hidden_gradient)[0].astype(jnp.bfloat16)

    d_mod = own_slot(contract_cols(d_pre, full_up).astype(jnp.bfloat16))
    grad_up = own_grads(contract_rows(mod_in, d_pre))
    branch = own_slot(contract_cols(hidden, full_down).astype(jnp.bfloat16))
    block_out = whole_sample((joined32 + gate * branch).astype(jnp.bfloat16), text)

    d_normed = d_mod * (1.0 + scale)
    d_full = d_out32 + inv_std * (
        d_normed
        - jnp.mean(d_normed, axis=-1, keepdims=True)
        - normed * jnp.mean(d_normed * normed, axis=-1, keepdims=True)
    )
    d_tokens = whole_sample(d_full.astype(jnp.bfloat16), text)

    null_rows = jnp.where(dropped, d_full[:text], jnp.float32(0.0))
    for axis, k in (("y", 1), ("y", 2), (Z, 1), (Z, 2)):
        null_rows = null_rows + peer(null_rows, axis, k)
    grad_null = all_slots(null_rows).reshape(text_len, width)
    return (block_out, d_tokens, grad_up, grad_down, grad_null)


def solution(mesh):
    torus = Mesh(
        mesh.devices.reshape(2, 2, 4, 4, 2, 2), ("zq", "zp", "y", "x", "zh", "c")
    )
    in_specs = (
        P(DP, None, None),
        P(DP, None, None),
        P(),
        P(DP),
        P(DP),
        P(),
        P(DP, MP),
        P(MP, DP),
        P(DP, None, None),
    )
    out_specs = (P(DP, None, None), P(DP, None, None), P(DP, MP), P(MP, DP), P())
    return jax.shard_map(
        shards, mesh=torus, in_specs=in_specs, out_specs=out_specs, check_vma=False
    )
```

```python
import jax
import jax.numpy as jnp
from jax import lax
from jax.sharding import Mesh
from jax.sharding import PartitionSpec as P

EPS = 1e-06


Z = ("zq", "zp")
DP = ("zq", "zp", "y")
MP = ("x", "zh", "c")
SIZE = {Z: 4, "y": 4, "x": 4, "zp": 2, "zh": 2, "c": 2}
SLOTS = 8


def peer(value, axis, k):
    return lax.ppermute(value, axis, [(i, i ^ k) for i in range(SIZE[axis])])


def gathered(value, axis):
    return [value] + [peer(value, axis, k) for k in range(1, SIZE[axis])]


def after(value, *others):
    return lax.optimization_barrier((value, *others))[0]


def ring_gathered(value, axis):
    up = [(i, (i + 1) % 4) for i in range(4)]
    down = [(i, (i - 1) % 4) for i in range(4)]
    left = lax.ppermute(value, axis, up)
    right = lax.ppermute(value, axis, down)
    half = value.shape[0] // 2
    first = lax.ppermute(left[:half], axis, up)
    second = lax.ppermute(right[half:], axis, down)
    return [value, right, jnp.concatenate([first, second], axis=0), left]


def ordered(pieces, axis):
    own = lax.axis_index(axis)
    return [lax.select_n(own ^ j, *pieces) if len(pieces) > 2 else
            jnp.where(own == j, pieces[0], pieces[1]) for j in range(len(pieces))]


def total(pieces):
    acc = pieces[0].astype(jnp.float32)
    for piece in pieces[1:]:
        acc = acc + piece.astype(jnp.float32)
    return acc


def rounded(value):
    return lax.reduce_precision(value, 8, 7).astype(jnp.bfloat16)


def gelu_tanh(values):
    return jax.nn.gelu(values, approximate=True)


def contract_rows(left, right):
    return lax.dot_general(
        left, right, (((0,), (0,)), ((), ())), preferred_element_type=jnp.float32
    )


def contract_cols(left, right):
    return lax.dot_general(
        left, right, (((1,), (1,)), ((), ())), preferred_element_type=jnp.float32
    )


def halves_by_z(weight):
    first = lax.axis_index("zp") == 0
    left, right = jnp.split(weight, 2, axis=1)
    mine = jnp.where(first, left, right)
    other = jnp.where(first, right, left)
    return [mine, peer(other, Z, 1), peer(mine, Z, 2), peer(other, Z, 3)]


def all_rows(by_z):
    by_y = ring_gathered(jnp.stack(ordered(by_z, Z)), "y")
    y = lax.axis_index("y")
    rows = [lax.select_n((j - y) & 3, *by_y) for j in range(4)]
    return jnp.concatenate(rows, axis=1).reshape(-1, by_z[0].shape[1])


def grads_by_y(grad):
    blocks = grad.astype(jnp.bfloat16).reshape(4, 4, -1, grad.shape[1])
    y = lax.axis_index("y")
    sent = [lax.dynamic_index_in_dim(blocks, y ^ k, 1, keepdims=False) for k in range(4)]
    return [sent[0]] + [peer(sent[k], "y", k) for k in range(1, 4)]


def grads_by_z(terms):
    block = rounded(total(terms))
    z = lax.axis_index(Z)
    sent = [lax.dynamic_index_in_dim(block, z ^ k, 0, keepdims=False) for k in range(4)]
    got = [sent[0]] + [peer(sent[k], Z, k) for k in range(1, 4)]
    return [got[0], got[2], got[1], got[3]]


def own_grads(terms):
    mine, other = total(terms[:2]), total(terms[2:])
    first = lax.axis_index("zp") == 0
    return jnp.concatenate([jnp.where(first, mine, other), jnp.where(first, other, mine)], axis=1)


def group_tokens(pair):
    along_x = jnp.concatenate(gathered(pair, "x"), axis=0)
    return jnp.concatenate(gathered(along_x, "c"), axis=0).reshape(-1, pair.shape[-1])


def over_core(part):
    halves = part.reshape(2, -1, part.shape[1])
    return [halves[0], peer(halves[1], "c", 1)]


def over_x(terms):
    half = rounded(total(terms)).reshape(4, -1, terms[0].shape[1])
    return half, [half[0]] + [peer(half[k], "x", k) for k in range(1, 4)]


def over_pair(terms):
    slot = rounded(total(terms)).reshape(2, -1, terms[0].shape[1])
    return [slot[0], peer(slot[1], "zp", 1)]


def over_z_hi(terms):
    own = rounded(total(terms))
    return own, [own, peer(own, "zh", 1)]


def all_slots(rows):
    along_x = jnp.stack(ordered(gathered(rows, "x"), "x"))
    return jnp.concatenate(ordered(gathered(along_x, "c"), "c"), axis=0)


def whole_sample(rows, text):
    every = all_slots(rows)
    width = rows.shape[1]
    return jnp.concatenate(
        [every[:, :text].reshape(-1, width), every[:, text:].reshape(-1, width)], axis=0
    )[None]


def shards(
    image_tokens,
    text_tokens,
    null_prompt,
    drop_flags,
    time_index,
    modulation,
    w_up,
    w_down,
    d_output,
):
    text_len, width = null_prompt.shape
    text = text_len // SLOTS
    image = image_tokens.shape[1] // SLOTS
    place = lax.axis_index(("c", "x"))
    dropped = drop_flags[0] == 1

    up_by_z = halves_by_z(w_up)
    full_up = all_rows(up_by_z)

    def rows_of(array, start, count):
        return lax.dynamic_slice_in_dim(array, start, count, 0)

    joined32 = jnp.concatenate(
        [
            jnp.where(
                dropped,
                rows_of(null_prompt, place * text, text),
                rows_of(text_tokens[0], place * text, text),
            ),
            rows_of(image_tokens[0], place * image, image),
        ],
        axis=0,
    ).astype(jnp.float32)
    d_out32 = jnp.concatenate(
        [
            rows_of(d_output[0], place * text, text),
            rows_of(d_output[0], text_len + place * image, image),
        ],
        axis=0,
    ).astype(jnp.float32)
    vectors = lax.dynamic_index_in_dim(modulation, time_index[0], 0, keepdims=False)
    shift, scale, gate = vectors[0][None], vectors[1][None], vectors[2][None]
    centred = joined32 - jnp.mean(joined32, axis=-1, keepdims=True)
    inv_std = lax.rsqrt(jnp.mean(centred * centred, axis=-1, keepdims=True) + EPS)
    normed = centred * inv_std
    mod_slot = (normed * (1.0 + scale) + shift).astype(jnp.bfloat16)
    back_slot = (d_out32 * gate).astype(jnp.bfloat16)

    mod_pair = jnp.stack([mod_slot, peer(mod_slot, "zp", 1)])
    back_pair = jnp.stack([back_slot, peer(back_slot, "zp", 1)])
    mod_in = group_tokens(mod_pair)
    d_branch = group_tokens(back_pair)
    full_down = all_rows(halves_by_z(w_down.T))

    pre = jnp.dot(mod_in, full_up, preferred_element_type=jnp.float32)
    hidden = gelu_tanh(pre).astype(jnp.bfloat16)
    hidden_gradient = jnp.dot(d_branch, full_down, preferred_element_type=jnp.float32)
    _, gelu_back = jax.vjp(gelu_tanh, pre)
    d_pre = gelu_back(hidden_gradient)[0].astype(jnp.bfloat16)

    d_part = contract_cols(d_pre, full_up).astype(jnp.bfloat16)
    d_core = over_core(d_part)
    down_grad = contract_rows(d_branch, after(hidden, d_part)).astype(jnp.bfloat16)
    down_y = grads_by_y(down_grad)
    part = contract_cols(after(hidden, down_grad), full_down).astype(jnp.bfloat16)
    core = over_core(part)
    d_half, d_x = over_x(d_core)
    half, x = over_x([after(core[0], d_half), core[1]])
    up_y = grads_by_y(contract_rows(mod_in, after(d_pre, half)).astype(jnp.bfloat16))

    d_own, d_z_hi = over_z_hi(over_pair(d_x))
    own, z_hi = over_z_hi(over_pair(x))
    d_mod = total(d_z_hi)
    d_normed = d_mod * (1.0 + scale)
    d_full = d_out32 + inv_std * (
        d_normed
        - jnp.mean(d_normed, axis=-1, keepdims=True)
        - normed * jnp.mean(d_normed * normed, axis=-1, keepdims=True)
    )
    null_rows = jnp.where(dropped, d_full[:text], jnp.float32(0.0))
    null_rows = null_rows + peer(null_rows, Z, 1)
    d_rows = d_full.astype(jnp.bfloat16)
    d_tokens = whole_sample(d_rows, text)
    branch = total([after(z_hi[0], d_rows), z_hi[1]])
    block_out = whole_sample((joined32 + gate * branch).astype(jnp.bfloat16), text)
    down_z = grads_by_z([after(down_y[0], null_rows)] + down_y[1:])
    null_rows = null_rows + peer(null_rows, Z, 2)
    up_z = grads_by_z([after(up_y[0], null_rows, down_z[0])] + up_y[1:])
    null_rows = null_rows + peer(null_rows, "y", 1)
    null_rows = null_rows + peer(null_rows, "y", 2)
    grad_null = all_slots(null_rows).reshape(text_len, width)
    grad_down = own_grads([after(down_z[0], null_rows)] + down_z[1:]).T
    grad_up = own_grads(up_z)
    return (block_out, d_tokens, grad_up, grad_down, grad_null)


def solution(mesh):
    torus = Mesh(
        mesh.devices.reshape(2, 2, 4, 4, 2, 2), ("zq", "zp", "y", "x", "zh", "c")
    )
    in_specs = (
        P(DP, None, None),
        P(DP, None, None),
        P(),
        P(DP),
        P(DP),
        P(),
        P(DP, MP),
        P(MP, DP),
        P(DP, None, None),
    )
    out_specs = (P(DP, None, None), P(DP, None, None), P(DP, MP), P(MP, DP), P())
    return jax.shard_map(
        shards, mesh=torus, in_specs=in_specs, out_specs=out_specs, check_vma=False
    )
```

```python
import jax
import jax.numpy as jnp
from jax import lax
from jax.experimental import pallas as pl
from jax.experimental.pallas import tpu as pltpu
from jax.sharding import Mesh
from jax.sharding import PartitionSpec as P


EPS = 1e-06


Z = ("zq", "zp")
DP = ("zq", "zp", "y")
MP = ("x", "zh", "c")
SIZE = {Z: 4, "y": 4, "x": 4, "zp": 2, "zh": 2, "c": 2}
SLOTS = 8


def peer(value, axis, k):
    return lax.ppermute(value, axis, [(i, i ^ k) for i in range(SIZE[axis])])


def gathered(value, axis):
    return [value] + [peer(value, axis, k) for k in range(1, SIZE[axis])]


def after(value, *others):
    return lax.optimization_barrier((value, *others))[0]


def ring_gathered(value, axis):
    up = [(i, (i + 1) % 4) for i in range(4)]
    down = [(i, (i - 1) % 4) for i in range(4)]
    left = lax.ppermute(value, axis, up)
    right = lax.ppermute(value, axis, down)
    half = value.shape[0] // 2
    first = lax.ppermute(left[:half], axis, up)
    second = lax.ppermute(right[half:], axis, down)
    return value, right, first, second, left


def ordered(pieces, axis):
    own = lax.axis_index(axis)
    return [lax.select_n(own ^ j, *pieces) if len(pieces) > 2 else
            jnp.where(own == j, pieces[0], pieces[1]) for j in range(len(pieces))]


def total(pieces):
    acc = pieces[0].astype(jnp.float32)
    for piece in pieces[1:]:
        acc = acc + piece.astype(jnp.float32)
    return acc


def rounded(value):
    return lax.reduce_precision(value, 8, 7).astype(jnp.bfloat16)


def gelu_tanh(values):
    return jax.nn.gelu(values, approximate=True)


def all_weights(weights):
    first = lax.axis_index("zp") == 0
    left, right = jnp.split(weights, 2, axis=2)
    mine = jnp.where(first, left, right)
    other = jnp.where(first, right, left)
    by_z = [mine] + [peer(v, Z, k) for k, v in ((1, other), (2, mine), (3, other))]
    return ring_gathered(jnp.stack(ordered(by_z, Z), axis=1), "y")


def inner_kernel(y_ref, near, far, own, following, over_up, over_down, before, inner, w, acc):
    z = pl.program_id(0)
    pieces = (
        (own[0, 0], own[1, 0]),
        (following[0, 0], following[1, 0]),
        (over_up[0, 0], over_down[0, 0]),
        (before[0, 0], before[1, 0]),
    )
    rows = own.shape[2]
    for place, pair in enumerate(pieces):
        start = pl.multiple_of(((y_ref[0] + place) & 3) * rows, rows)
        for t in range(2):
            w[t, pl.ds(start, rows), :] = pair[t]

    @pl.when(z == 0)
    def _():
        acc[...] = jnp.zeros_like(acc)

    half = acc.shape[1] // 2
    for t in range(2):
        for c, source in enumerate((near, far)):
            acc[t, c * half : (c + 1) * half, :] += jnp.dot(
                source[:, t].reshape(half, -1), w[t], preferred_element_type=jnp.float32
            )

    @pl.when(z == pl.num_programs(0) - 1)
    def _():
        def chunk(at, carry):
            part = pl.ds(pl.multiple_of(at * 32, 32), 32)
            hidden, back = jax.vjp(gelu_tanh, acc[0, part, :])
            inner[0, part, :] = back(acc[1, part, :])[0].astype(jnp.bfloat16)
            inner[1, part, :] = hidden.astype(jnp.bfloat16)
            return carry

        lax.fori_loop(0, acc.shape[1] // 32, chunk, 0)


def parts_kernel(inner, w, d_keep, d_send, keep, send):
    half = inner.shape[1] // 2
    for t, outs in enumerate(((d_keep, d_send), (keep, send))):
        for c, out in enumerate(outs):
            out[...] = lax.dot_general(
                inner[t, c * half : (c + 1) * half, :],
                w[t],
                (((1,), (1,)), ((), ())),
                preferred_element_type=jnp.float32,
            ).astype(jnp.bfloat16)


def grads_kernel(y_ref, near, far, inner, out0, out1, out2, out3, both):
    half = inner.shape[1] // 2
    rows = out0.shape[2]
    for t in range(2):
        terms = [
            lax.dot_general(
                source[:, t].reshape(half, -1),
                inner[t, c * half : (c + 1) * half, :],
                (((0,), (0,)), ((), ())),
                preferred_element_type=jnp.float32,
            )
            for c, source in enumerate((near, far))
        ]
        both[...] = (terms[0] + terms[1]).astype(jnp.bfloat16)
        for k, out in enumerate((out0, out1, out2, out3)):
            start = pl.multiple_of((y_ref[0] ^ k) * rows, rows)
            out[t, 0] = both[pl.ds(start, rows), :]


def whole(shape):
    return pl.BlockSpec(shape, lambda z, *_: (0,) * len(shape))


def cost(tokens, width, hid, nbytes):
    return pl.CostEstimate(
        flops=4 * tokens * width * hid, transcendentals=0, bytes_accessed=nbytes
    )


def products(y, near, far, pieces, interpret=False):
    width = near.shape[-1]
    tokens = 2 * near.size // (2 * width)
    rows, hid = pieces[0].shape[2:]
    block = width // 4
    token_spec = pl.BlockSpec((*near.shape[:-1], block), lambda z, *_: (0, 0, 0, 0, z))
    two = pl.BlockSpec((2, 1, rows, hid), lambda z, *_: (0, z, 0, 0))
    one = pl.BlockSpec((1, 1, rows, hid), lambda z, *_: (0, z, 0, 0))
    w_spec = pl.BlockSpec((2, block, hid), lambda z, *_: (0, z, 0))
    inner_shape = jax.ShapeDtypeStruct((2, tokens, hid), jnp.bfloat16)
    estimate = cost(tokens, width, hid, 4 * near.size * 2)
    inner, w = pl.pallas_call(
        inner_kernel,
        out_shape=(inner_shape, jax.ShapeDtypeStruct((2, width, hid), jnp.bfloat16)),
        grid_spec=pltpu.PrefetchScalarGridSpec(
            num_scalar_prefetch=1,
            grid=(4,),
            in_specs=[token_spec, token_spec, two, two, one, one, two],
            out_specs=(whole(inner_shape.shape), w_spec),
            scratch_shapes=[pltpu.VMEM((2, tokens, hid), jnp.float32)],
        ),
        cost_estimate=estimate,
        name="inner",
        interpret=interpret,
    )(y, near, far, *pieces)
    part_spec = pl.BlockSpec((tokens // 2, block), lambda z: (0, z))
    parts = pl.pallas_call(
        parts_kernel,
        out_shape=(jax.ShapeDtypeStruct((tokens // 2, width), jnp.bfloat16),) * 4,
        grid=(4,),
        in_specs=[whole(inner.shape), w_spec],
        out_specs=(part_spec,) * 4,
        cost_estimate=estimate,
        name="parts",
        interpret=interpret,
    )(inner, w)
    inner = after(inner, *parts)
    grads = pl.pallas_call(
        grads_kernel,
        out_shape=(jax.ShapeDtypeStruct((2, 4, rows, hid), jnp.bfloat16),) * 4,
        grid_spec=pltpu.PrefetchScalarGridSpec(
            num_scalar_prefetch=1,
            grid=(4,),
            in_specs=[token_spec, token_spec, whole(inner.shape)],
            out_specs=(two,) * 4,
            scratch_shapes=[pltpu.VMEM((block, hid), jnp.bfloat16)],
        ),
        cost_estimate=estimate,
        name="grads",
        interpret=interpret,
    )(y, near, far, inner)
    return parts, grads


def grads_by_z(terms):
    block = rounded(total(terms))
    z = lax.axis_index(Z)
    sent = [
        jnp.stack([lax.dynamic_index_in_dim(b, z ^ k, 0, keepdims=False) for b in block])
        for k in range(4)
    ]
    got = [sent[0]] + [peer(sent[k], Z, k) for k in range(1, 4)]
    return [got[0], got[2], got[1], got[3]]


def own_grads(terms):
    mine, other = total(terms[:2]), total(terms[2:])
    first = lax.axis_index("zp") == 0
    return [
        jnp.concatenate([jnp.where(first, m, o), jnp.where(first, o, m)], axis=1)
        for m, o in zip(mine, other)
    ]


def over_x(terms):
    half = rounded(total(terms)).reshape(4, -1, terms[0].shape[1])
    return half, [half[0]] + [peer(half[k], "x", k) for k in range(1, 4)]


def over_pair(terms):
    slot = rounded(total(terms)).reshape(2, -1, terms[0].shape[1])
    return [slot[0], peer(slot[1], "zp", 1)]


def over_z_hi(terms):
    own = rounded(total(terms))
    return [own, peer(own, "zh", 1)]


def all_slots(rows):
    along_x = jnp.stack(ordered(gathered(rows, "x"), "x"))
    return jnp.concatenate(ordered(gathered(along_x, "c"), "c"), axis=0)


def whole_sample(rows, text):
    every = all_slots(rows)
    width = rows.shape[1]
    return jnp.concatenate(
        [every[:, :text].reshape(-1, width), every[:, text:].reshape(-1, width)], axis=0
    )[None]


def shards(
    image_tokens,
    text_tokens,
    null_prompt,
    drop_flags,
    time_index,
    modulation,
    w_up,
    w_down,
    d_output,
):
    text_len, width = null_prompt.shape
    text = text_len // SLOTS
    image = image_tokens.shape[1] // SLOTS
    place = lax.axis_index(("c", "x"))
    dropped = drop_flags[0] == 1

    pieces = all_weights(jnp.stack([w_up, w_down.T]))

    def rows_of(array, start, count):
        return lax.dynamic_slice_in_dim(array, start, count, 0)

    joined32 = jnp.concatenate(
        [
            jnp.where(
                dropped,
                rows_of(null_prompt, place * text, text),
                rows_of(text_tokens[0], place * text, text),
            ),
            rows_of(image_tokens[0], place * image, image),
        ],
        axis=0,
    ).astype(jnp.float32)
    d_out32 = jnp.concatenate(
        [
            rows_of(d_output[0], place * text, text),
            rows_of(d_output[0], text_len + place * image, image),
        ],
        axis=0,
    ).astype(jnp.float32)
    vectors = lax.dynamic_index_in_dim(modulation, time_index[0], 0, keepdims=False)
    shift, scale, gate = vectors[0][None], vectors[1][None], vectors[2][None]
    centred = joined32 - jnp.mean(joined32, axis=-1, keepdims=True)
    inv_std = lax.rsqrt(jnp.mean(centred * centred, axis=-1, keepdims=True) + EPS)
    normed = centred * inv_std
    mod_slot = (normed * (1.0 + scale) + shift).astype(jnp.bfloat16)
    back_slot = (d_out32 * gate).astype(jnp.bfloat16)

    both = jnp.stack([mod_slot, back_slot])
    pairs = gathered(jnp.stack([both, peer(both, "zp", 1)], axis=1), "x")
    near = jnp.stack([after(pairs[0], pieces[1], pieces[4])] + pairs[1:])
    far = peer(near, "c", 1)

    parts, grads = products(lax.axis_index("y")[None], near, far, pieces)
    d_keep, d_send, keep, send = parts

    d_half, d_x = over_x([d_keep, peer(d_send, "c", 1)])
    grads_y = [grads[0]] + [peer(grads[k], "y", k) for k in range(1, 4)]
    _, x = over_x([after(keep, d_half), peer(send, "c", 1)])

    d_own, d_other = over_z_hi(over_pair(d_x))
    pair = over_pair([after(x[0], d_own)] + x[1:])
    d_mod = total([d_own, d_other])
    d_normed = d_mod * (1.0 + scale)
    d_full = d_out32 + inv_std * (
        d_normed
        - jnp.mean(d_normed, axis=-1, keepdims=True)
        - normed * jnp.mean(d_normed * normed, axis=-1, keepdims=True)
    )
    null_rows = jnp.where(dropped, d_full[:text], jnp.float32(0.0))
    null_rows = null_rows + peer(null_rows, Z, 1)
    d_rows = d_full.astype(jnp.bfloat16)
    d_tokens = whole_sample(d_rows, text)
    own, other = over_z_hi(pair)
    null_rows = null_rows + peer(null_rows, Z, 2)
    branch = total([own, after(other, null_rows)])
    out_rows = (joined32 + gate * branch).astype(jnp.bfloat16)
    block_out = whole_sample(out_rows, text)
    null_rows = null_rows + peer(null_rows, "y", 1)
    grads_z = grads_by_z([after(grads_y[0], out_rows, null_rows)] + grads_y[1:])
    null_rows = null_rows + peer(null_rows, "y", 2)
    grad_null = all_slots(null_rows).reshape(text_len, width)
    grad_up, grad_down = own_grads(grads_z)
    grad_down = grad_down.T
    return (block_out, d_tokens, grad_up, grad_down, grad_null)


def solution(mesh):
    torus = Mesh(
        mesh.devices.reshape(2, 2, 4, 4, 2, 2), ("zq", "zp", "y", "x", "zh", "c")
    )
    in_specs = (
        P(DP, None, None),
        P(DP, None, None),
        P(),
        P(DP),
        P(DP),
        P(),
        P(DP, MP),
        P(MP, DP),
        P(DP, None, None),
    )
    out_specs = (P(DP, None, None), P(DP, None, None), P(DP, MP), P(MP, DP), P())
    return jax.shard_map(
        shards, mesh=torus, in_specs=in_specs, out_specs=out_specs, check_vma=False
    )
```

```python
import jax
import jax.numpy as jnp
from jax import lax
from jax.sharding import Mesh
from jax.sharding import PartitionSpec as P


EPS = 1e-06


Z = ("zq", "zp")
DP = ("zq", "zp", "y")
MP = ("x", "zh", "c")
SIZE = {Z: 4, "y": 4, "x": 4, "zp": 2, "zh": 2, "c": 2}
SLOTS = 8


def peer(value, axis, k):
    return lax.ppermute(value, axis, [(i, i ^ k) for i in range(SIZE[axis])])


def gathered(value, axis):
    return [value] + [peer(value, axis, k) for k in range(1, SIZE[axis])]


def after(value, *others):
    return lax.optimization_barrier((value, *others))[0]


def ring_gathered(value, axis):
    up = [(i, (i + 1) % 4) for i in range(4)]
    down = [(i, (i - 1) % 4) for i in range(4)]
    left = lax.ppermute(value, axis, up)
    right = lax.ppermute(value, axis, down)
    half = value.shape[0] // 2
    first = lax.ppermute(left[:half], axis, up)
    second = lax.ppermute(right[half:], axis, down)
    return [value, right, jnp.concatenate([first, second], axis=0), left]


def ordered(pieces, axis):
    own = lax.axis_index(axis)
    return [lax.select_n(own ^ j, *pieces) if len(pieces) > 2 else
            jnp.where(own == j, pieces[0], pieces[1]) for j in range(len(pieces))]


def total(pieces):
    acc = pieces[0].astype(jnp.float32)
    for piece in pieces[1:]:
        acc = acc + piece.astype(jnp.float32)
    return acc


def rounded(value):
    return lax.reduce_precision(value, 8, 7).astype(jnp.bfloat16)


def gelu_tanh(values):
    return jax.nn.gelu(values, approximate=True)


def contract_rows(left, right):
    return lax.dot_general(
        left, right, (((0,), (0,)), ((), ())), preferred_element_type=jnp.float32
    )


def contract_cols(left, right):
    return lax.dot_general(
        left, right, (((1,), (1,)), ((), ())), preferred_element_type=jnp.float32
    )


def halves_by_z(weight):
    first = lax.axis_index("zp") == 0
    left, right = jnp.split(weight, 2, axis=1)
    mine = jnp.where(first, left, right)
    other = jnp.where(first, right, left)
    return [mine] + [peer(v, Z, k) for k, v in ((1, other), (2, mine), (3, other))]


def all_rows(by_z):
    by_y = ring_gathered(jnp.stack(ordered(by_z, Z)), "y")
    y = lax.axis_index("y")
    rows = [lax.select_n((j - y) & 3, *by_y) for j in range(4)]
    return jnp.concatenate(rows, axis=1).reshape(-1, by_z[0].shape[1])


RING = {
    "up": [(i, (i + 1) % 4) for i in range(4)],
    "down": [(i, (i - 1) % 4) for i in range(4)],
}


def grads_by_y(grads):
    blocks = [grad.reshape(4, 4, -1, grad.shape[1]) for grad in grads]
    y = lax.axis_index("y")

    def rows_for(k):
        place = (y + k) & 3
        return [lax.dynamic_index_in_dim(b, place, 1, keepdims=False) for b in blocks]

    mine, following, over, before = (rows_for(k) for k in range(4))
    first = lax.ppermute(over[0], "y", RING["up"])
    second = lax.ppermute(over[1], "y", RING["down"])
    up = jnp.stack([rounded(total([following[0], first])), following[1]])
    down = jnp.stack([before[0], rounded(total([before[1], second]))])
    return [
        jnp.stack(mine), lax.ppermute(up, "y", RING["up"]), lax.ppermute(down, "y", RING["down"])
    ]


def grads_by_z(terms):
    block = rounded(total(terms))
    z = lax.axis_index(Z)
    sent = [
        jnp.stack([lax.dynamic_index_in_dim(b, z ^ k, 0, keepdims=False) for b in block])
        for k in range(4)
    ]
    got = [sent[0]] + [peer(sent[k], Z, k) for k in range(1, 4)]
    return [got[0], got[2], got[1], got[3]]


def own_grads(terms):
    mine, other = total(terms[:2]), total(terms[2:])
    first = lax.axis_index("zp") == 0
    return [
        jnp.concatenate([jnp.where(first, m, o), jnp.where(first, o, m)], axis=1)
        for m, o in zip(mine, other)
    ]


def group_tokens(own, partner):
    along_x = jnp.stack([own, jnp.stack(gathered(partner, "x"), axis=1)], axis=1)
    whole = jnp.stack(gathered(along_x, "c"), axis=1)
    return [tensor.reshape(-1, own.shape[-1]) for tensor in whole]


def over_core(part):
    halves = part.reshape(2, -1, part.shape[1])
    return [halves[0], peer(halves[1], "c", 1)]


def over_x(terms):
    half = rounded(total(terms)).reshape(2, 4, -1, terms[0].shape[1])
    return half, [half[:, 0]] + [peer(half[:, k], "x", k) for k in range(1, 4)]


def over_pair(terms):
    slot = rounded(total(terms))
    return [slot[0], peer(slot[1], "zp", 1)]


def over_z_hi(terms):
    own = rounded(total(terms))
    return [own, peer(own, "zh", 1)]


def all_slots(rows):
    along_x = jnp.stack(ordered(gathered(rows, "x"), "x"))
    return jnp.concatenate(ordered(gathered(along_x, "c"), "c"), axis=0)


def whole_sample(rows, text):
    every = all_slots(rows)
    width = rows.shape[1]
    return jnp.concatenate(
        [every[:, :text].reshape(-1, width), every[:, text:].reshape(-1, width)], axis=0
    )[None]


def shards(
    image_tokens,
    text_tokens,
    null_prompt,
    drop_flags,
    time_index,
    modulation,
    w_up,
    w_down,
    d_output,
):
    text_len, width = null_prompt.shape
    text = text_len // SLOTS
    image = image_tokens.shape[1] // SLOTS
    dropped = drop_flags[0] == 1

    full_up = all_rows(halves_by_z(w_up))
    full_down = all_rows(halves_by_z(w_down.T))

    def rows_of(array, start, count):
        return lax.dynamic_slice_in_dim(array, start, count, 0)

    def slot_of(k):
        place = lax.axis_index("c") * 4 + (lax.axis_index("x") ^ k)
        joined = [
            jnp.where(
                dropped,
                rows_of(null_prompt, place * text, text),
                rows_of(text_tokens[0], place * text, text),
            ),
            rows_of(image_tokens[0], place * image, image),
        ]
        d_out = [
            rows_of(d_output[0], place * text, text),
            rows_of(d_output[0], text_len + place * image, image),
        ]
        return [jnp.concatenate(rows, axis=0).astype(jnp.float32) for rows in (joined, d_out)]

    def normalized(rows):
        centred = rows - jnp.mean(rows, axis=-1, keepdims=True)
        inv_std = lax.rsqrt(jnp.mean(centred * centred, axis=-1, keepdims=True) + EPS)
        return centred * inv_std, inv_std

    vectors = lax.dynamic_index_in_dim(modulation, time_index[0], 0, keepdims=False)
    shift, scale, gate = vectors[0][None], vectors[1][None], vectors[2][None]

    def inputs_of(normed, d_out):
        return jnp.stack(
            [
                (normed * (1.0 + scale) + shift).astype(jnp.bfloat16),
                (d_out * gate).astype(jnp.bfloat16),
            ]
        )

    joined32, d_out32 = slot_of(0)
    normed, inv_std = normalized(joined32)
    both = inputs_of(normed, d_out32)
    partner = peer(both, "zp", 1)
    others = [slot_of(k) for k in range(1, 4)]
    rest = inputs_of(
        normalized(jnp.concatenate([rows for rows, _ in others], axis=0))[0],
        jnp.concatenate([rows for _, rows in others], axis=0),
    )
    own = jnp.concatenate([both, rest], axis=1).reshape(2, 4, -1, width)
    mod_in, d_branch = group_tokens(own, partner)

    pre = jnp.dot(mod_in, full_up, preferred_element_type=jnp.float32)
    hidden = gelu_tanh(pre).astype(jnp.bfloat16)
    hidden_gradient = jnp.dot(d_branch, full_down, preferred_element_type=jnp.float32)
    _, gelu_back = jax.vjp(gelu_tanh, pre)
    d_pre = gelu_back(hidden_gradient)[0].astype(jnp.bfloat16)

    d_part = contract_cols(d_pre, full_up).astype(jnp.bfloat16)
    d_core = over_core(d_part)
    part = contract_cols(after(hidden, d_part), full_down).astype(jnp.bfloat16)
    core = over_core(part)
    d_half, d_x = over_x(d_core)
    down_grad = contract_rows(d_branch, after(hidden, part, d_half)).astype(jnp.bfloat16)
    up_grad = contract_rows(mod_in, after(d_pre, part, d_half)).astype(jnp.bfloat16)
    grads_y = grads_by_y([up_grad, down_grad])
    _, x = over_x([after(core[0], down_grad, up_grad), core[1]])

    d_own, d_other = over_z_hi(over_pair(d_x))
    pair = over_pair([after(x[0], d_own)] + x[1:])
    d_mod = total([d_own, d_other])
    d_normed = d_mod * (1.0 + scale)
    d_full = d_out32 + inv_std * (
        d_normed
        - jnp.mean(d_normed, axis=-1, keepdims=True)
        - normed * jnp.mean(d_normed * normed, axis=-1, keepdims=True)
    )
    null_rows = jnp.where(dropped, d_full[:text], jnp.float32(0.0))
    null_rows = null_rows + peer(null_rows, Z, 1)
    d_rows = d_full.astype(jnp.bfloat16)
    d_tokens = whole_sample(d_rows, text)
    own, other = over_z_hi(pair)
    grads_z = grads_by_z([after(grads_y[0], null_rows)] + grads_y[1:])
    far_null = peer(null_rows, Z, 2)
    branch = total([own, after(other, d_rows)])
    out_rows = (joined32 + gate * branch).astype(jnp.bfloat16)
    block_out = whole_sample(out_rows, text)
    null_rows = null_rows + after(far_null, grads_z[0])
    null_rows = null_rows + peer(null_rows, "y", 1)
    null_rows = null_rows + peer(null_rows, "y", 2)
    grad_null = all_slots(null_rows).reshape(text_len, width)
    grad_up, grad_down = own_grads(grads_z)
    grad_down = grad_down.T
    return (block_out, d_tokens, grad_up, grad_down, grad_null)


def solution(mesh):
    torus = Mesh(
        mesh.devices.reshape(2, 2, 4, 4, 2, 2), ("zq", "zp", "y", "x", "zh", "c")
    )
    in_specs = (
        P(DP, None, None),
        P(DP, None, None),
        P(),
        P(DP),
        P(DP),
        P(),
        P(DP, MP),
        P(MP, DP),
        P(DP, None, None),
    )
    out_specs = (P(DP, None, None), P(DP, None, None), P(DP, MP), P(MP, DP), P())
    return jax.shard_map(
        shards, mesh=torus, in_specs=in_specs, out_specs=out_specs, check_vma=False
    )
```

```python
import jax
import jax.numpy as jnp
from jax import lax
from jax.sharding import Mesh
from jax.sharding import PartitionSpec as P


EPS = 1e-06


Z = ("zq", "zp")
DP = ("zq", "zp", "y")
MP = ("x", "zh", "c")
SIZE = {Z: 4, "y": 4, "x": 4, "zp": 2, "zh": 2, "c": 2}
SLOTS = 8


def peer(value, axis, k):
    return lax.ppermute(value, axis, [(i, i ^ k) for i in range(SIZE[axis])])


def gathered(value, axis):
    return [value] + [peer(value, axis, k) for k in range(1, SIZE[axis])]


def after(value, *others):
    return lax.optimization_barrier((value, *others))[0]


def ring_gathered(value, axis):
    up = [(i, (i + 1) % 4) for i in range(4)]
    down = [(i, (i - 1) % 4) for i in range(4)]
    left = lax.ppermute(value, axis, up)
    right = lax.ppermute(value, axis, down)
    half = value.shape[0] // 2
    first = lax.ppermute(left[:half], axis, up)
    second = lax.ppermute(right[half:], axis, down)
    return [value, right, jnp.concatenate([first, second], axis=0), left]


def ordered(pieces, axis):
    own = lax.axis_index(axis)
    return [lax.select_n(own ^ j, *pieces) if len(pieces) > 2 else
            jnp.where(own == j, pieces[0], pieces[1]) for j in range(len(pieces))]


def total(pieces):
    acc = pieces[0].astype(jnp.float32)
    for piece in pieces[1:]:
        acc = acc + piece.astype(jnp.float32)
    return acc


def rounded(value):
    return lax.reduce_precision(value, 8, 7).astype(jnp.bfloat16)


def gelu_tanh(values):
    return jax.nn.gelu(values, approximate=True)


def contract_rows(left, right):
    return lax.dot_general(
        left, right, (((0,), (0,)), ((), ())), preferred_element_type=jnp.float32
    )


def contract_cols(left, right):
    return lax.dot_general(
        left, right, (((1,), (1,)), ((), ())), preferred_element_type=jnp.float32
    )


def halves_by_z(weight):
    first = lax.axis_index("zp") == 0
    left, right = jnp.split(weight, 2, axis=1)
    mine = jnp.where(first, left, right)
    other = jnp.where(first, right, left)
    return [mine] + [peer(v, Z, k) for k, v in ((1, other), (2, mine), (3, other))]


def all_rows(by_z):
    by_y = ring_gathered(jnp.stack(ordered(by_z, Z)), "y")
    y = lax.axis_index("y")
    rows = [lax.select_n((j - y) & 3, *by_y) for j in range(4)]
    return jnp.concatenate(rows, axis=1).reshape(-1, by_z[0].shape[1])


RING = {
    "up": [(i, (i + 1) % 4) for i in range(4)],
    "down": [(i, (i - 1) % 4) for i in range(4)],
}


def grads_by_y(grads):
    blocks = [grad.reshape(4, 4, -1, grad.shape[1]) for grad in grads]
    y = lax.axis_index("y")

    def rows_for(k):
        place = (y + k) & 3
        return [lax.dynamic_index_in_dim(b, place, 1, keepdims=False) for b in blocks]

    mine, following, over, before = (rows_for(k) for k in range(4))
    first = lax.ppermute(over[0], "y", RING["up"])
    second = lax.ppermute(over[1], "y", RING["down"])
    up = jnp.stack([rounded(total([following[0], first])), following[1]])
    down = jnp.stack([before[0], rounded(total([before[1], second]))])
    return [
        jnp.stack(mine), lax.ppermute(up, "y", RING["up"]), lax.ppermute(down, "y", RING["down"])
    ]


def grads_by_z(terms):
    block = rounded(total(terms))
    z = lax.axis_index(Z)
    sent = [
        jnp.stack([lax.dynamic_index_in_dim(b, z ^ k, 0, keepdims=False) for b in block])
        for k in range(4)
    ]
    got = [sent[0]] + [peer(sent[k], Z, k) for k in range(1, 4)]
    return [got[0], got[2], got[1], got[3]]


def own_grads(terms):
    mine, other = total(terms[:2]), total(terms[2:])
    first = lax.axis_index("zp") == 0
    return [
        jnp.concatenate([jnp.where(first, m, o), jnp.where(first, o, m)], axis=1)
        for m, o in zip(mine, other)
    ]


def group_tokens(own, partner):
    along_x = jnp.stack([own, jnp.stack(gathered(partner, "x"), axis=1)], axis=1)
    whole = jnp.stack(gathered(along_x, "c"), axis=1)
    return [tensor.reshape(-1, own.shape[-1]) for tensor in whole]


def over_core(parts):
    half = parts[0].shape[0] // 2
    got = peer(jnp.stack([part[half:] for part in parts]), "c", 1)
    return [[part[:half], term] for part, term in zip(parts, got)]


def over_x(terms):
    half = rounded(total(terms)).reshape(2, 4, -1, terms[0].shape[1])
    return half, [half[:, 0]] + [peer(half[:, k], "x", k) for k in range(1, 4)]


def over_pair(terms):
    slot = rounded(total(terms))
    return [slot[0], peer(slot[1], "zp", 1)]


def over_z_hi(terms):
    own = rounded(total(terms))
    return [own, peer(own, "zh", 1)]


def x_slots(rows):
    return jnp.stack(ordered(gathered(rows, "x"), "x"))


def all_slots(along_x):
    return jnp.concatenate(ordered(gathered(along_x, "c"), "c"), axis=-3)


def whole_sample(every, text):
    width = every.shape[-1]
    return jnp.concatenate(
        [every[:, :text].reshape(-1, width), every[:, text:].reshape(-1, width)], axis=0
    )[None]


def shards(
    image_tokens,
    text_tokens,
    null_prompt,
    drop_flags,
    time_index,
    modulation,
    w_up,
    w_down,
    d_output,
):
    text_len, width = null_prompt.shape
    text = text_len // SLOTS
    image = image_tokens.shape[1] // SLOTS
    dropped = drop_flags[0] == 1

    full_up = all_rows(halves_by_z(w_up))
    full_down = all_rows(halves_by_z(w_down.T))

    def rows_of(array, start, count):
        return lax.dynamic_slice_in_dim(array, start, count, 0)

    def slot_of(k):
        place = lax.axis_index("c") * 4 + (lax.axis_index("x") ^ k)
        joined = [
            jnp.where(
                dropped,
                rows_of(null_prompt, place * text, text),
                rows_of(text_tokens[0], place * text, text),
            ),
            rows_of(image_tokens[0], place * image, image),
        ]
        d_out = [
            rows_of(d_output[0], place * text, text),
            rows_of(d_output[0], text_len + place * image, image),
        ]
        return [jnp.concatenate(rows, axis=0).astype(jnp.float32) for rows in (joined, d_out)]

    def normalized(rows):
        centred = rows - jnp.mean(rows, axis=-1, keepdims=True)
        inv_std = lax.rsqrt(jnp.mean(centred * centred, axis=-1, keepdims=True) + EPS)
        return centred * inv_std, inv_std

    vectors = lax.dynamic_index_in_dim(modulation, time_index[0], 0, keepdims=False)
    shift, scale, gate = vectors[0][None], vectors[1][None], vectors[2][None]

    def inputs_of(normed, d_out):
        return jnp.stack(
            [
                (normed * (1.0 + scale) + shift).astype(jnp.bfloat16),
                (d_out * gate).astype(jnp.bfloat16),
            ]
        )

    joined32, d_out32 = slot_of(0)
    normed, inv_std = normalized(joined32)
    both = inputs_of(normed, d_out32)
    partner = peer(both, "zp", 1)
    others = [slot_of(k) for k in range(1, 4)]
    rest = inputs_of(
        normalized(jnp.concatenate([rows for rows, _ in others], axis=0))[0],
        jnp.concatenate([rows for _, rows in others], axis=0),
    )
    own = jnp.concatenate([both, rest], axis=1).reshape(2, 4, -1, width)
    mod_in, d_branch = group_tokens(own, partner)

    pre = jnp.dot(mod_in, full_up, preferred_element_type=jnp.float32)
    hidden = gelu_tanh(pre).astype(jnp.bfloat16)
    hidden_gradient = jnp.dot(d_branch, full_down, preferred_element_type=jnp.float32)
    _, gelu_back = jax.vjp(gelu_tanh, pre)
    d_pre = gelu_back(hidden_gradient)[0].astype(jnp.bfloat16)

    d_part = contract_cols(d_pre, full_up).astype(jnp.bfloat16)
    part = contract_cols(after(hidden, d_part), full_down).astype(jnp.bfloat16)
    d_core, core = over_core([d_part, part])
    d_half, d_x = over_x(d_core)
    down_grad = contract_rows(d_branch, after(hidden, part, d_half)).astype(jnp.bfloat16)
    up_grad = contract_rows(mod_in, after(d_pre, part, d_half)).astype(jnp.bfloat16)
    grads_y = grads_by_y([up_grad, down_grad])
    _, x = over_x([after(core[0], down_grad, up_grad), core[1]])

    d_own, d_other = over_z_hi(over_pair(d_x))
    pair = over_pair([after(x[0], d_own)] + x[1:])
    d_mod = total([d_own, d_other])
    d_normed = d_mod * (1.0 + scale)
    d_full = d_out32 + inv_std * (
        d_normed
        - jnp.mean(d_normed, axis=-1, keepdims=True)
        - normed * jnp.mean(d_normed * normed, axis=-1, keepdims=True)
    )
    null_rows = jnp.where(dropped, d_full[:text], jnp.float32(0.0))
    null_rows = null_rows + peer(null_rows, Z, 1)
    d_rows = d_full.astype(jnp.bfloat16)
    d_slots = x_slots(d_rows)
    own, other = over_z_hi(pair)
    grads_z = grads_by_z([after(grads_y[0], null_rows)] + grads_y[1:])
    far_null = peer(null_rows, Z, 2)
    branch = total([own, after(other, d_rows)])
    out_rows = (joined32 + gate * branch).astype(jnp.bfloat16)
    out_slots = x_slots(out_rows)
    null_rows = null_rows + after(far_null, grads_z[0])
    null_rows = null_rows + peer(null_rows, "y", 1)
    null_rows = null_rows + peer(null_rows, "y", 2)
    every = all_slots(jnp.stack([d_slots, out_slots]))
    d_tokens, block_out = [whole_sample(rows, text) for rows in every]
    grad_null = all_slots(x_slots(null_rows)).reshape(text_len, width)
    grad_up, grad_down = own_grads(grads_z)
    grad_down = grad_down.T
    return (block_out, d_tokens, grad_up, grad_down, grad_null)


def solution(mesh):
    torus = Mesh(
        mesh.devices.reshape(2, 2, 4, 4, 2, 2), ("zq", "zp", "y", "x", "zh", "c")
    )
    in_specs = (
        P(DP, None, None),
        P(DP, None, None),
        P(),
        P(DP),
        P(DP),
        P(),
        P(DP, MP),
        P(MP, DP),
        P(DP, None, None),
    )
    out_specs = (P(DP, None, None), P(DP, None, None), P(DP, MP), P(MP, DP), P())
    return jax.shard_map(
        shards, mesh=torus, in_specs=in_specs, out_specs=out_specs, check_vma=False
    )
```
